32 devices in a mesh: dp: 2 (over x), ctx: 4 (over y, core), tp: 4 (over z).
Axes of the slice: x: 2, y: 2, z: 4, core: 2. Of those that a mesh axis runs over, the one named last changes fastest.
Arguments:
- block_input: bfloat16 [2, 8, 256, 2048], P('dp', 'ctx', 'tp'), may hold values from -6 to 6
- block_order: int32 [2, 8], P('dp'), may hold values from 0 to 7, each once within a row
- w_qkv: bfloat16 [2048, 3, 2048], P(('dp', 'ctx'), None, 'tp'), may hold values from -1 to 1
- w_out: bfloat16 [2048, 2048], P('tp', ('dp', 'ctx')), may hold values from -3 to 3
- gain_attn: bfloat16 [2048], P(('dp', 'ctx')), may hold values from 0.5 to 1.5
- w_gate_up: bfloat16 [2048, 2, 8192], P(('dp', 'ctx'), None, 'tp'), may hold values from -0.125 to 0.125
- w_down: bfloat16 [8192, 2048], P('tp', ('dp', 'ctx')), may hold values from -0.0625 to 0.0625
- gain_mlp: bfloat16 [2048], P(('dp', 'ctx')), may hold values from 0.5 to 1.5
- cotangent: bfloat16 [2, 8, 256, 2048], P('dp', 'ctx', 'tp'), may hold values from -6 to 6
Outputs:
- block_output: bfloat16 [2, 8, 256, 2048], P('dp', 'ctx', 'tp')
- input_grad: float32 [2, 8, 256, 2048], P('dp', 'ctx', 'tp')
- grad_qkv: float32 [2048, 3, 2048], P(('dp', 'ctx'), None, 'tp')
- grad_out: float32 [2048, 2048], P('tp', ('dp', 'ctx'))
- grad_gain_attn: float32 [2048], P(('dp', 'ctx'))
- grad_gate_up: float32 [2048, 2, 8192], P(('dp', 'ctx'), None, 'tp')
- grad_down: float32 [8192, 2048], P('tp', ('dp', 'ctx'))
- grad_gain_mlp: float32 [2048], P(('dp', 'ctx'))
The draws below stay inside these ranges and needn't reach their ends.
Inputs may be any that keep to these rules, and one draw needn't show every extreme that they name: `block_order`: each row lists every block number of one sequence once.
All inputs are finite; a program needn't handle non-finite values.
Results may differ from the reference program's by a relative error of at most 0.019.
Values may be sent and summed in bfloat16 or wider, within the bound.
A program may use at most 192 MiB of HBM per device.

```python
import jax
import jax.numpy as jnp
from jax import lax

D = 2048
N_HEADS = 32
HEAD_DIM = 64
FF = 8192
BLOCK = 256
BLOCKS = 8
SEQUENCES = 2


def draw_w_qkv(key, part):
    first = jax.random.fold_in(jax.random.fold_in(key, 11), 0)
    base = jax.random.normal(first, (D, 3, D), jnp.float32) * D ** (-0.5)
    return jnp.clip(base, -1.0, 1.0).astype(jnp.bfloat16)


def block_levels(stream_key, shape, cuts, low, top_value):
    def one(dim, shards_of):
        steps = jax.random.uniform(jax.random.fold_in(jax.random.fold_in(stream_key, 6), dim), (shards_of,), jnp.float32, low / len(cuts), top_value / len(cuts))
        return jnp.repeat(jnp.exp(steps), shape[dim] // shards_of).reshape((-1,) + (1,) * (len(shape) - dim - 1))

    loudness = one(*cuts[0])
    for cut in cuts[1:]:
        loudness = loudness * one(*cut)
    return loudness


def noise(key, extent, deviation, bound, shards=(), held_as=jnp.bfloat16):
    result = deviation * jax.random.normal(key, extent, jnp.float32)
    if shards:
        result = result * block_levels(key, extent, shards, -0.22, 0.18)
    return jnp.clip(result, -bound, bound).astype(held_as)


def setup_inputs(seed: int = 0) -> dict:
    seeds = jax.random.split(jax.random.key(seed), 10)
    block_input = noise(seeds[0], (SEQUENCES, BLOCKS, BLOCK, D), 1.0, 6.0, ((0, 2), (1, 4), (2, 4)))
    block_order = jax.vmap(lambda own: jax.random.permutation(own, BLOCKS))(jax.random.split(seeds[1], SEQUENCES)).reshape((SEQUENCES, BLOCKS)).astype(jnp.int32)
    w_qkv = draw_w_qkv(jax.random.fold_in(seeds[9], 71), 0)
    w_out = noise(seeds[3], (D, D), 4 ** -0.5, 3.0, ((0, 4), (1, 8)))
    gain_attn = jnp.clip(1.0 + 0.1 * jax.random.normal(seeds[4], (D,), jnp.float32), 0.5, 1.5).astype(jnp.bfloat16)
    w_gate_up = noise(seeds[5], (D, 2, FF), D ** -0.5, 0.125, ((0, 8), (2, 4)))
    w_down = noise(seeds[6], (FF, D), FF ** -0.5, 0.0625, ((0, 4), (1, 8)))
    gain_mlp = jnp.clip(1.0 + 0.1 * jax.random.normal(seeds[7], (D,), jnp.float32), 0.5, 1.5).astype(jnp.bfloat16)
    cotangent = noise(seeds[8], (SEQUENCES, BLOCKS, BLOCK, D), 1.0, 6.0, ((0, 2), (1, 4), (2, 4)))
    return {"block_input": block_input, "block_order": block_order, "w_qkv": w_qkv, "w_out": w_out, "gain_attn": gain_attn, "w_gate_up": w_gate_up, "w_down": w_down, "gain_mlp": gain_mlp, "cotangent": cotangent}


EPSILON = 1e-05
ROPE_BASE = 130000.0

def rope_tables(positions, head_size):
    half = head_size // 2
    freq = ROPE_BASE ** (-(jnp.arange(half, dtype=jnp.float32) * 2.0 / head_size))
    angle = positions.astype(jnp.float32)[..., None] * freq
    cosine = jnp.cos(angle)
    sine = jnp.sin(angle)
    return (jnp.concatenate([cosine, cosine], -1), jnp.concatenate([sine, sine], -1))

def rotate(values):
    half = values.shape[-1] // 2
    return jnp.concatenate([-values[..., half:], values[..., :half]], -1)

def unrotate(values):
    half = values.shape[-1] // 2
    return jnp.concatenate([values[..., half:], -values[..., :half]], -1)

def rope_apply(values, cosine, sine):
    return values * cosine + rotate(values) * sine

def rope_back(grads, cosine, sine):
    return grads * cosine + unrotate(grads * sine)

def reference(block_input, block_order, w_qkv, w_out, gain_attn, w_gate_up, w_down, gain_mlp, cotangent):
    f32 = jnp.float32
    bf16 = jnp.bfloat16
    highest = lax.Precision.HIGHEST
    length = BLOCK * BLOCKS
    query_rows = min(512, length)
    block_count = length // query_rows
    gain_one = gain_attn.astype(f32)
    gain_two = gain_mlp.astype(f32)
    qkv_flat = w_qkv.reshape(D, 3 * D)
    gate_up_flat = w_gate_up.reshape(D, 2 * FF)

    def per_sequence(totals, packed):
        inputs, cotan, group_ids = packed
        offsets = jnp.arange(BLOCK, dtype=jnp.int32)
        positions = (group_ids[:, None] * BLOCK + offsets[None, :]).reshape(length).astype(jnp.int32)
        cosine, sine = rope_tables(positions, HEAD_DIM)
        cosine = cosine[:, None, :]
        sine = sine[:, None, :]
        x_float = inputs.reshape(length, D).astype(f32)
        rms_attn = lax.rsqrt(lax.optimization_barrier(jnp.mean(x_float * x_float, -1, keepdims=True)) + EPSILON)
        unit_attn = x_float * rms_attn
        normed_attn = (unit_attn * gain_one).astype(bf16)
        qkv = jnp.dot(normed_attn, qkv_flat, preferred_element_type=f32).reshape(length, 3, N_HEADS, HEAD_DIM)
        queries = (rope_apply(qkv[:, 0], cosine, sine) * 0.125).astype(bf16)
        keys = rope_apply(qkv[:, 1], cosine, sine).astype(bf16)
        values = qkv[:, 2].astype(bf16)
        queries, keys, values = lax.optimization_barrier((queries, keys, values))
        key_float = keys.astype(f32)
        value_float = values.astype(f32)
        query_blocks = queries.reshape(block_count, query_rows, N_HEADS, HEAD_DIM)
        position_blocks = positions.reshape(block_count, query_rows)

        def block_scores(query_blk, query_pos):
            scores = jnp.einsum('qhe,khe->hqk', query_blk.astype(f32), key_float, precision=highest)
            visible = positions[None, :] <= query_pos[:, None]
            return jnp.where(visible[None], scores, -jnp.inf)

        def attend(packed_block):
            query_blk, query_pos = packed_block
            scores = block_scores(query_blk, query_pos)
            row_max = lax.optimization_barrier(jnp.max(scores, -1, keepdims=True))
            log_total = row_max + jnp.log(lax.optimization_barrier(jnp.sum(jnp.exp(scores - row_max), -1, keepdims=True)))
            probs = jnp.exp(scores - log_total)
            mixed = jnp.einsum('hqk,khe->qhe', probs, value_float, precision=highest)
            return (mixed.astype(bf16), log_total[..., 0])
        attn_blocks, log_totals = lax.map(attend, (query_blocks, position_blocks))
        attn_blocks = lax.optimization_barrier(attn_blocks)
        attention = attn_blocks.reshape(length, D)
        resid_mid = x_float + jnp.dot(attention, w_out, preferred_element_type=f32)
        rms_mlp = lax.rsqrt(lax.optimization_barrier(jnp.mean(resid_mid * resid_mid, -1, keepdims=True)) + EPSILON)
        unit_mlp = resid_mid * rms_mlp
        normed_mlp = (unit_mlp * gain_two).astype(bf16)
        gate_up = jnp.dot(normed_mlp, gate_up_flat, preferred_element_type=f32).reshape(length, 2, FF)
        gate = gate_up[:, 0]
        upper = gate_up[:, 1]
        sigma = jax.nn.sigmoid(gate)
        hidden = (gate * sigma * upper).astype(bf16)
        resid_out = resid_mid + jnp.dot(hidden, w_down, preferred_element_type=f32)
        block_output = resid_out.astype(bf16)
        cotan_flat = cotan.reshape(length, D)
        grad_down = jnp.dot(hidden.T, cotan_flat, preferred_element_type=f32)
        grad_hidden = jnp.dot(cotan_flat, w_down.T, preferred_element_type=f32)
        act_grad = jnp.stack([grad_hidden * upper * sigma * (1.0 + gate * (1.0 - sigma)), grad_hidden * gate * sigma], 1).astype(bf16)
        act_flat = act_grad.reshape(length, 2 * FF)
        grad_gate_up = jnp.dot(normed_mlp.T, act_flat, preferred_element_type=f32).reshape(D, 2, FF)
        grad_normed_mlp = jnp.dot(act_flat, gate_up_flat.T, preferred_element_type=f32)
        grad_gain_mlp = lax.optimization_barrier(jnp.sum(grad_normed_mlp * unit_mlp, 0))
        scaled_two = grad_normed_mlp * gain_two
        grad_mid = cotan_flat.astype(f32) + rms_mlp * (scaled_two - unit_mlp * lax.optimization_barrier(jnp.mean(scaled_two * unit_mlp, -1, keepdims=True)))
        grad_mid_b = grad_mid.astype(bf16)
        grad_out = jnp.dot(attention.T, grad_mid_b, preferred_element_type=f32)
        grad_attention = jnp.dot(grad_mid_b, w_out.T, preferred_element_type=f32).astype(bf16)
        grad_attention = lax.optimization_barrier(grad_attention)
        grad_blocks = grad_attention.reshape(block_count, query_rows, N_HEADS, HEAD_DIM)

        def back_block(carry, packed_block):
            grad_keys, grad_values = carry
            query_blk, query_pos, log_total, grad_blk, attn_blk = packed_block
            scores = block_scores(query_blk, query_pos)
            probs = jnp.exp(scores - log_total[..., None])
            delta = lax.optimization_barrier(jnp.sum(grad_blk.astype(f32) * attn_blk.astype(f32), -1)).T
            dprobs = jnp.einsum('qhe,khe->hqk', grad_blk.astype(f32), value_float, precision=highest)
            grad_scores = lax.optimization_barrier((probs * (dprobs - delta[..., None])).astype(bf16)).astype(f32)
            probs_b = lax.optimization_barrier(probs.astype(bf16)).astype(f32)
            grad_query = jnp.einsum('hqk,khe->qhe', grad_scores, key_float, precision=highest)
            grad_keys = grad_keys + jnp.einsum('hqk,qhe->khe', grad_scores, query_blk.astype(f32), precision=highest)
            grad_values = grad_values + jnp.einsum('hqk,qhe->khe', probs_b, grad_blk.astype(f32), precision=highest)
            return ((grad_keys, grad_values), grad_query)
        zeros = jnp.zeros((length, N_HEADS, HEAD_DIM), f32)
        (grad_keys, grad_values), grad_queries = lax.scan(back_block, (zeros, zeros), (query_blocks, position_blocks, log_totals, grad_blocks, attn_blocks))
        grad_queries = grad_queries.reshape(length, N_HEADS, HEAD_DIM)
        qkv_grad = jnp.stack([rope_back(grad_queries, cosine, sine) * 0.125, rope_back(grad_keys, cosine, sine), grad_values], 1).astype(bf16)
        qkv_grad = qkv_grad.reshape(length, 3 * D)
        grad_qkv = jnp.dot(normed_attn.T, qkv_grad, preferred_element_type=f32).reshape(D, 3, D)
        grad_normed_attn = jnp.dot(qkv_grad, qkv_flat.T, preferred_element_type=f32)
        grad_gain_attn = lax.optimization_barrier(jnp.sum(grad_normed_attn * unit_attn, 0))
        scaled_one = grad_normed_attn * gain_one
        input_grad = grad_mid + rms_attn * (scaled_one - unit_attn * lax.optimization_barrier(jnp.mean(scaled_one * unit_attn, -1, keepdims=True)))
        new_totals = (totals[0] + grad_qkv, totals[1] + grad_out, totals[2] + grad_gain_attn, totals[3] + grad_gate_up, totals[4] + grad_down, totals[5] + grad_gain_mlp)
        return (new_totals, (block_output.reshape(BLOCKS, BLOCK, D), input_grad.reshape(BLOCKS, BLOCK, D)))
    start = (jnp.zeros((D, 3, D), f32), jnp.zeros((D, D), f32), jnp.zeros((D,), f32), jnp.zeros((D, 2, FF), f32), jnp.zeros((FF, D), f32), jnp.zeros((D,), f32))
    totals, (outputs, input_grads) = lax.scan(per_sequence, start, (block_input, cotangent, block_order))
    return (outputs, input_grads, totals[0], totals[1], totals[2], totals[3], totals[4], totals[5])
```

```python
import functools

import jax
import jax.numpy as jnp
from jax import lax
from jax.experimental import pallas as pl
from jax.experimental.pallas import tpu as pltpu
from jax.sharding import PartitionSpec as P

HEAD_DIM = 64
PAIR = 2 * HEAD_DIM
NT = (((1,), (1,)), ((), ()))
NN = (((1,), (0,)), ((), ()))
TN = (((0,), (0,)), ((), ()))


def dot(a, b, dims):
    return lax.dot_general(a, b, dims, preferred_element_type=jnp.float32)


def swap_halves(x):
    lane = lax.broadcasted_iota(jnp.int32, x.shape, 1)
    half = HEAD_DIM // 2
    return jnp.where(
        lane % HEAD_DIM < half, pltpu.roll(x, PAIR - half, 1), pltpu.roll(x, half, 1)
    )


def head_part(x, head):
    lane = lax.broadcasted_iota(jnp.int32, x.shape, 1)
    return jnp.where(lane // HEAD_DIM == head, x, jnp.zeros_like(x))


def visible(shape, base, key_off, key_id, query_id, span):
    keys = lax.broadcasted_iota(jnp.int32, shape, 0)
    queries = lax.broadcasted_iota(jnp.int32, shape, 1)
    return keys - queries <= (query_id - key_id) * span


def attend_kernel(order_ref, mine_ref, q_ref, k_ref, v_ref, o_ref, lse_ref, s_ref):
    blocks, span, _ = k_ref.shape
    rows = q_ref.shape[0]
    parts = rows // span

    def one(index, carry):
        head = index // parts
        part = index % parts
        start = pl.multiple_of(part * span, span)
        query = head_part(q_ref[pl.ds(start, span), :], head)
        top = jnp.full((8, span), -1e30, jnp.float32)
        for blk in range(blocks):
            s = dot(k_ref[blk], query, NT)
            seen = visible((span, span), 0, 0, order_ref[blk], mine_ref[part], span)
            s = jnp.where(seen, s, -jnp.inf)
            s_ref[blk] = s
            top = jnp.maximum(top, jnp.max(s.reshape(span // 8, 8, span), 0))
        top = jnp.max(top, 0, keepdims=True)
        total = jnp.zeros((8, span), jnp.float32)
        acc = jnp.zeros((PAIR, span), jnp.float32)
        for blk in range(blocks):
            p = jnp.exp(s_ref[blk] - top)
            total = total + jnp.sum(p.reshape(span // 8, 8, span), 0)
            acc = acc + dot(v_ref[blk], p.astype(jnp.bfloat16), TN)
        total = jnp.sum(total, 0, keepdims=True)
        out = (acc / total).T
        lane = lax.broadcasted_iota(jnp.int32, out.shape, 1)
        old = o_ref[pl.ds(start, span), :]
        o_ref[pl.ds(start, span), :] = jnp.where(
            lane // HEAD_DIM == head, out.astype(o_ref.dtype), old
        )
        lse_ref[0, pl.ds(head * parts + part, 1), :] = top + jnp.log(total)
        return carry

    lax.fori_loop(0, 2 * parts, one, 0)


def attend(order, mine, q, k, v):
    rows, width = q.shape
    blocks, span, _ = k.shape
    pairs = width // PAIR
    parts = rows // span
    return pl.pallas_call(
        attend_kernel,
        out_shape=(
            jax.ShapeDtypeStruct((rows, width), jnp.bfloat16),
            jax.ShapeDtypeStruct((pairs, 2 * parts, span), jnp.float32),
        ),
        grid_spec=pltpu.PrefetchScalarGridSpec(
            num_scalar_prefetch=2,
            grid=(pairs,),
            in_specs=[
                pl.BlockSpec((rows, PAIR), lambda i, *_: (0, i)),
                pl.BlockSpec((blocks, span, PAIR), lambda i, *_: (0, 0, i)),
                pl.BlockSpec((blocks, span, PAIR), lambda i, *_: (0, 0, i)),
            ],
            out_specs=[
                pl.BlockSpec((rows, PAIR), lambda i, *_: (0, i)),
                pl.BlockSpec((1, 2 * parts, span), lambda i, *_: (i, 0, 0)),
            ],
            scratch_shapes=[pltpu.VMEM((blocks, span, span), jnp.float32)],
        ),
        cost_estimate=pl.CostEstimate(
            flops=4 * rows * blocks * span * width * 4,
            bytes_accessed=4 * blocks * span * width + 4 * rows * width,
            transcendentals=rows * blocks * span * width // HEAD_DIM,
        ),
        name="attend",
    )(order, mine, q, k, v)


def attend_back_kernel(
    order_ref, mine_ref, q_ref, k_ref, v_ref, o_ref, g_ref, lse_ref, cos_ref, sin_ref,
    qcos_ref, qsin_ref, dq_ref, dk_ref, dv_ref, dk_acc, dv_acc, dq_acc, kt_ref, delta_ref,
):
    blocks, span, _ = k_ref.shape
    rows = q_ref.shape[0]
    parts = rows // span
    f32 = jnp.float32
    bf16 = jnp.bfloat16
    for blk in range(blocks):
        kt_ref[blk] = k_ref[blk].T
        dk_acc[blk] = jnp.zeros((span, PAIR), f32)
        dv_acc[blk] = jnp.zeros((span, PAIR), f32)
    for part in range(parts):
        take = pl.ds(part * span, span)
        both = (g_ref[take, :].astype(f32) * o_ref[take, :].astype(f32)).T
        for head in range(2):
            delta_ref[pl.ds(head * parts + part, 1), :] = jnp.sum(
                both[head * HEAD_DIM : (head + 1) * HEAD_DIM], 0, keepdims=True
            )
        dq_acc[part] = jnp.zeros((PAIR, span), f32)

    def one(index, carry):
        head = index // parts
        part = index % parts
        start = pl.multiple_of(part * span, span)
        query = head_part(q_ref[pl.ds(start, span), :], head)
        grad = head_part(g_ref[pl.ds(start, span), :], head)
        lse = lse_ref[0, pl.ds(index, 1), :]
        delta = delta_ref[pl.ds(index, 1), :]
        dq = jnp.zeros((PAIR, span), f32)
        for blk in range(blocks):
            s = dot(k_ref[blk], query, NT)
            seen = visible((span, span), 0, 0, order_ref[blk], mine_ref[part], span)
            p = jnp.exp(jnp.where(seen, s - lse, -jnp.inf))
            dp = dot(v_ref[blk], grad, NT)
            ds = (p * (dp - delta)).astype(bf16)
            dv_acc[blk] += dot(p.astype(bf16), grad, NN)
            dk_acc[blk] += dot(ds, query, NN)
            dq = dq + dot(kt_ref[blk], ds, NN)
        sub = lax.broadcasted_iota(jnp.int32, dq.shape, 0)
        dq_acc[part] += jnp.where(sub // HEAD_DIM == head, dq, 0.0)
        return carry

    lax.fori_loop(0, 2 * parts, one, 0)
    for part in range(parts):
        take = pl.ds(part * span, span)
        dq = dq_acc[part].T
        dq = dq * qcos_ref[take, :] - swap_halves(dq) * qsin_ref[take, :]
        dq_ref[take, :] = (dq * 0.125).astype(bf16)
    for blk in range(blocks):
        dk = dk_acc[blk]
        dk = dk * cos_ref[blk] - swap_halves(dk) * sin_ref[blk]
        dk_ref[blk] = dk.astype(bf16)
        dv_ref[blk] = dv_acc[blk].astype(bf16)


def attend_back(order, mine, q, k, v, o, g, lse, cos, sin, qcos, qsin):
    rows, width = q.shape
    blocks, span, _ = k.shape
    pairs = width // PAIR
    parts = rows // span
    row_spec = pl.BlockSpec((rows, PAIR), lambda i, *_: (0, i))
    blk_spec = pl.BlockSpec((blocks, span, PAIR), lambda i, *_: (0, 0, i))
    tab_spec = pl.BlockSpec((blocks, span, PAIR), lambda i, *_: (0, 0, 0))
    qtab_spec = pl.BlockSpec((rows, PAIR), lambda i, *_: (0, 0))
    f32 = jnp.float32
    return pl.pallas_call(
        attend_back_kernel,
        out_shape=(
            jax.ShapeDtypeStruct((rows, width), jnp.bfloat16),
            jax.ShapeDtypeStruct((blocks, span, width), jnp.bfloat16),
            jax.ShapeDtypeStruct((blocks, span, width), jnp.bfloat16),
        ),
        grid_spec=pltpu.PrefetchScalarGridSpec(
            num_scalar_prefetch=2,
            grid=(pairs,),
            in_specs=[
                row_spec, blk_spec, blk_spec, row_spec, row_spec,
                pl.BlockSpec((1, 2 * parts, span), lambda i, *_: (i, 0, 0)),
                tab_spec, tab_spec, qtab_spec, qtab_spec,
            ],
            out_specs=[row_spec, blk_spec, blk_spec],
            scratch_shapes=[
                pltpu.VMEM((blocks, span, PAIR), f32),
                pltpu.VMEM((blocks, span, PAIR), f32),
                pltpu.VMEM((parts, PAIR, span), f32),
                pltpu.VMEM((blocks, PAIR, span), jnp.bfloat16),
                pltpu.VMEM((2 * parts, span), f32),
            ],
        ),
        cost_estimate=pl.CostEstimate(
            flops=10 * rows * blocks * span * width * 4,
            bytes_accessed=8 * blocks * span * width + 8 * rows * width,
            transcendentals=rows * blocks * span * width // HEAD_DIM,
        ),
        name="attend_back",
    )(order, mine, q, k, v, o, g, lse, cos, sin, qcos, qsin)


def project_kernel(x_ref, w_ref, cos_ref, sin_ref, q_ref, k_ref, v_ref):
    which = pl.program_id(0)
    out = dot(x_ref[...], w_ref[...], NN)

    def turned(scale, ref):
        for lane in range(0, out.shape[1], PAIR):
            piece = out[:, lane : lane + PAIR]
            piece = piece * cos_ref[...] + swap_halves(piece) * sin_ref[...]
            ref[:, lane : lane + PAIR] = (piece * scale).astype(ref.dtype)

    @pl.when(which == 0)
    def _():
        turned(0.125, q_ref)

    @pl.when(which == 1)
    def _():
        turned(1.0, k_ref)

    @pl.when(which == 2)
    def _():
        v_ref[...] = out.astype(v_ref.dtype)


def project(x, w, qcos, qsin):
    rows, depth = x.shape
    width = w.shape[1] // 3
    whole = lambda shape: pl.BlockSpec(shape, lambda t: (0,) * len(shape))
    out = jax.ShapeDtypeStruct((rows, width), jnp.bfloat16)
    return pl.pallas_call(
        project_kernel,
        out_shape=(out, out, out),
        grid=(3,),
        in_specs=[
            whole((rows, depth)),
            pl.BlockSpec((depth, width), lambda t: (0, t)),
            whole((rows, PAIR)),
            whole((rows, PAIR)),
        ],
        out_specs=[whole((rows, width))] * 3,
        cost_estimate=pl.CostEstimate(
            flops=2 * rows * depth * 3 * width,
            bytes_accessed=2 * depth * 3 * width + 2 * rows * depth,
            transcendentals=0,
        ),
        name="project",
    )(x, w, qcos, qsin)


def neighbour_barrier(line_axis, cube_axis):
    sem = pltpu.get_barrier_semaphore()
    count = 0
    if line_axis is not None:
        me = lax.axis_index(line_axis)
        size = lax.axis_size(line_axis)

        @pl.when(me > 0)
        def _():
            pl.semaphore_signal(sem, inc=1, device_id={line_axis: me - 1}, device_id_type=MESH)

        @pl.when(me < size - 1)
        def _():
            pl.semaphore_signal(sem, inc=1, device_id={line_axis: me + 1}, device_id_type=MESH)

    if cube_axis is not None:
        for bit in cube_bits(lax.axis_size(cube_axis)):
            pl.semaphore_signal(
                sem, inc=1, device_id={cube_axis: flipped(lax.axis_index(cube_axis), bit)},
                device_id_type=MESH,
            )
            count += 1
    if line_axis is not None:

        @pl.when((me > 0) & (me < size - 1))
        def _():
            pl.semaphore_wait(sem, count + 2)

        @pl.when((me == 0) | (me == size - 1))
        def _():
            pl.semaphore_wait(sem, count + 1)

    else:
        pl.semaphore_wait(sem, count)


def cube_bits(size):
    bits = []
    while size > 1:
        size //= 2
        bits.append(size)
    return bits


def flipped(index, bit):
    return index + bit - 2 * bit * ((index // bit) % 2)


def flip_all(index, mask):
    bit = 1
    while bit <= mask:
        if mask // bit % 2:
            index = flipped(index, bit)
        bit *= 2
    return index


def remote(src, dst, send, recv, axis, target):
    return pltpu.make_async_remote_copy(
        src_ref=src, dst_ref=dst, send_sem=send, recv_sem=recv,
        device_id={axis: target}, device_id_type=MESH,
    )


def row_gather_steps(axis, x_ref, o_ref, send, recv, local):
    size = lax.axis_size(axis)
    me = lax.axis_index(axis)
    pieces = x_ref.shape[0]
    own = [
        pltpu.make_async_copy(x_ref.at[p], o_ref.at[p, me], local.at[p]) for p in range(pieces)
    ]

    def copy(way, step, p):
        block = me - step if way == 0 else me + step
        src = x_ref.at[p] if step == 0 else o_ref.at[p, block]
        return remote(
            src, o_ref.at[p, block], send.at[way, step, p], recv.at[way, step, p],
            axis, me + 1 if way == 0 else me - 1,
        )

    def sends(way, step):
        if way == 0:
            return (me < size - 1) & (me - step >= 0)
        return (me > 0) & (me + step < size)

    def arrives(way, step):
        return me - 1 - step >= 0 if way == 0 else me + 1 + step < size

    def arrival(way, step, p):
        block = me - 1 - step if way == 0 else me + 1 + step
        return remote(
            o_ref.at[p, block], o_ref.at[p, block], send.at[way, step, p],
            recv.at[way, step, p], axis, me - 1 if way == 0 else me + 1,
        )

    for step in range(size):
        for p in range(pieces):
            for way in (0, 1):
                if step > 0:

                    @pl.when(arrives(way, step - 1))
                    def _(way=way, p=p):
                        arrival(way, step - 1, p).wait_recv()

                if step < size - 1:

                    @pl.when(sends(way, step))
                    def _(way=way, p=p):
                        copy(way, step, p).start()

        if step == 0:
            for one in own:
                one.start()
        yield
    for one in own:
        one.wait()
    for step in range(size - 1):
        for way in (0, 1):

            @pl.when(sends(way, step))
            def _(way=way):
                for p in range(pieces):
                    copy(way, step, p).wait_send()


def row_gather_scratch(size, pieces):
    return [
        pltpu.SemaphoreType.DMA((2, size - 1, pieces)),
        pltpu.SemaphoreType.DMA((2, size - 1, pieces)),
        pltpu.SemaphoreType.DMA((pieces,)),
    ]


def row_scatter_steps(axis, part_ref, o_ref, inbox, outbox, send, recv):
    size = lax.axis_size(axis)
    me = lax.axis_index(axis)
    pieces = part_ref.shape[0]
    f32 = jnp.float32

    def target(way, step):
        return size - 1 - step if way == 0 else step

    def from_edge(way):
        return me == 0 if way == 0 else me == size - 1

    def passes(way, step):
        dest = target(way, step)
        return dest > me if way == 0 else dest < me

    def arrives(way, step):
        dest = target(way, step)
        return (me > 0) & (dest >= me) if way == 0 else (me < size - 1) & (dest <= me)

    def copy(way, step, p, edge):
        src = part_ref.at[p, target(way, step)] if edge else outbox.at[way, step, p]
        return remote(
            src, inbox.at[way, step, p], send.at[way, step, p], recv.at[way, step, p],
            axis, me + 1 if way == 0 else me - 1,
        )

    def arrival(way, step, p):
        return remote(
            inbox.at[way, step, p], inbox.at[way, step, p], send.at[way, step, p],
            recv.at[way, step, p], axis, me - 1 if way == 0 else me + 1,
        )

    for step in range(size - 1):
        for p in range(pieces):
            for way in (0, 1):

                @pl.when(arrives(way, step))
                def _(way=way, p=p):
                    arrival(way, step, p).wait_recv()

                @pl.when(passes(way, step) & from_edge(way))
                def _(way=way, p=p):
                    copy(way, step, p, True).start()

                @pl.when(passes(way, step) & jnp.logical_not(from_edge(way)))
                def _(way=way, p=p):
                    outbox[way, step, p] = (
                        inbox[way, step, p].astype(f32)
                        + part_ref[p, target(way, step)].astype(f32)
                    ).astype(outbox.dtype)
                    copy(way, step, p, False).start()

        yield
    for p in range(pieces):
        own = part_ref[p, me].astype(f32)

        @pl.when(me == 0)
        def _(p=p, own=own):
            o_ref[p] = own + inbox[1, me, p].astype(f32)

        @pl.when(me == size - 1)
        def _(p=p, own=own):
            o_ref[p] = own + inbox[0, size - 1 - me, p].astype(f32)

        @pl.when((me > 0) & (me < size - 1))
        def _(p=p, own=own):
            o_ref[p] = own + (
                inbox[0, size - 1 - me, p].astype(f32) + inbox[1, me, p].astype(f32)
            )

    for step in range(size - 1):
        for way in (0, 1):

            @pl.when(passes(way, step))
            def _(way=way):
                for p in range(pieces):
                    copy(way, step, p, False).wait_send()


def row_scatter_scratch(size, block):
    pieces = block[0]
    return [
        pltpu.VMEM((2, size - 1) + block, jnp.bfloat16),
        pltpu.VMEM((2, size - 1) + block, jnp.bfloat16),
        pltpu.SemaphoreType.DMA((2, size - 1, pieces)),
        pltpu.SemaphoreType.DMA((2, size - 1, pieces)),
    ]


def cube_gather_steps(axis, x_refs, o_refs, send, recv, local):
    size = lax.axis_size(axis)
    me = lax.axis_index(axis)
    bits = cube_bits(size)
    count = len(x_refs)
    own = [
        pltpu.make_async_copy(x_refs[t], o_refs[t].at[me], local.at[t]) for t in range(count)
    ]

    def copy(mask, bit, t):
        block = flip_all(me, mask)
        src = x_refs[t] if mask == 0 else o_refs[t].at[block]
        return remote(
            src, o_refs[t].at[block], send.at[mask + bit, t], recv.at[mask + bit, t],
            axis, flipped(me, bit),
        )

    def arrival(mask, t):
        low = mask & -mask
        block = flip_all(me, mask)
        return remote(
            o_refs[t].at[block], o_refs[t].at[block], send.at[mask, t], recv.at[mask, t],
            axis, flipped(me, low),
        )

    waited = set()
    masks = [0]
    for bit in bits:
        for t in range(count):
            copy(0, bit, t).start()
    for one in own:
        one.start()
    yield
    for level, bit in enumerate(bits):
        for mask in masks:
            if mask == 0:
                continue
            for t in range(count):
                if (mask, t) not in waited:
                    arrival(mask, t).wait_recv()
                    waited.add((mask, t))
                copy(mask, bit, t).start()
        masks = masks + [mask + bit for mask in masks]
        yield
    for mask in masks:
        for t in range(count):
            if mask and (mask, t) not in waited:
                arrival(mask, t).wait_recv()
    for one in own:
        one.wait()
    for mask in masks:
        for t in range(count):
            if mask:
                low = mask & -mask
                copy(mask - low, low, t).wait_send()


def cube_gather_scratch(size, count):
    return [
        pltpu.SemaphoreType.DMA((size, count)),
        pltpu.SemaphoreType.DMA((size, count)),
        pltpu.SemaphoreType.DMA((count,)),
    ]


def cube_scatter_steps(axis, x_refs, o_refs, inbox, total, outbox, send, recv):
    size = lax.axis_size(axis)
    me = lax.axis_index(axis)
    bits = cube_bits(size)[::-1]
    count = len(x_refs)
    f32 = jnp.float32
    kept = list(range(size))[::-1]
    first = True
    for bit in bits:
        going = [mask for mask in kept if mask & bit]
        kept = [mask for mask in kept if not mask & bit]

        def copy(mask, t, bit=bit, first=first):
            src = x_refs[t].at[flip_all(me, mask)] if first else outbox.at[mask, t]
            return remote(
                src, inbox.at[mask, t], send.at[mask, t], recv.at[mask, t],
                axis, flipped(me, bit),
            )

        for mask in going:
            for t in range(count):
                if not first:
                    outbox[mask, t] = total[mask, t].astype(outbox.dtype)
                copy(mask, t).start()
        yield
        for mask in kept:
            for t in range(count):
                copy(mask + bit, t).wait_recv()
                if first:
                    base = x_refs[t][flip_all(me, mask)].astype(f32)
                else:
                    base = total[mask, t]
                total[mask, t] = base + inbox[mask + bit, t].astype(f32)
        for mask in going:
            for t in range(count):
                copy(mask, t).wait_send()
        first = False
    for t in range(count):
        o_refs[t][...] = total[0, t].astype(o_refs[t].dtype)


def cube_scatter_scratch(size, block, count):
    return [
        pltpu.VMEM((size, count) + block, jnp.bfloat16),
        pltpu.VMEM((size, count) + block, jnp.float32),
        pltpu.VMEM((size, count) + block, jnp.bfloat16),
        pltpu.SemaphoreType.DMA((size, count)),
        pltpu.SemaphoreType.DMA((size, count)),
    ]


def run_steps(*walks):
    walks = list(walks)
    while walks:
        for walk in list(walks):
            try:
                next(walk)
            except StopIteration:
                walks.remove(walk)


ANY = pl.BlockSpec(memory_space=pl.ANY)
IN_VMEM = pl.BlockSpec(memory_space=pltpu.VMEM)


def comm_params(number):
    return pltpu.CompilerParams(
        collective_id=number, has_side_effects=True, vmem_limit_bytes=48 * 1024 * 1024
    )


def comm_cost(size):
    return pl.CostEstimate(flops=0, bytes_accessed=size, transcendentals=0)


def gather_rows(x, number):
    pieces, rows, depth = x.shape
    size = lax.axis_size("tp")

    def kernel(x_ref, o_ref, send, recv, local):
        neighbour_barrier("tp", None)
        run_steps(row_gather_steps("tp", x_ref, o_ref, send, recv, local))

    return pl.pallas_call(
        kernel,
        out_shape=jax.ShapeDtypeStruct((pieces, size, rows, depth), x.dtype),
        in_specs=[IN_VMEM],
        out_specs=ANY,
        scratch_shapes=row_gather_scratch(size, pieces),
        compiler_params=comm_params(number),
        cost_estimate=comm_cost(COMM_BYTES),
        name="gather_rows",
    )(x)


def scatter_rows(part, number):
    pieces, size, rows, depth = part.shape

    def kernel(part_ref, o_ref, *scratch):
        neighbour_barrier("tp", None)
        run_steps(row_scatter_steps("tp", part_ref, o_ref, *scratch))

    return pl.pallas_call(
        kernel,
        out_shape=jax.ShapeDtypeStruct((pieces, rows, depth), jnp.float32),
        in_specs=[IN_VMEM],
        out_specs=IN_VMEM,
        scratch_shapes=row_scatter_scratch(size, (pieces, rows, depth)),
        compiler_params=comm_params(number),
        cost_estimate=comm_cost(COMM_BYTES),
        name="scatter_rows",
    )(part)


def gather_blocks(x, keys, values, number):
    pieces, rows, depth = x.shape
    size = lax.axis_size("tp")
    ring = lax.axis_size("ctx")

    def kernel(x_ref, k_ref, v_ref, o_ref, ko_ref, vo_ref, *sems):
        neighbour_barrier("tp", "ctx")
        run_steps(
            cube_gather_steps("ctx", (k_ref, v_ref), (ko_ref, vo_ref), *sems[3:]),
            row_gather_steps("tp", x_ref, o_ref, *sems[:3]),
        )

    blocks = jax.ShapeDtypeStruct((ring,) + keys.shape, keys.dtype)
    return pl.pallas_call(
        kernel,
        out_shape=(jax.ShapeDtypeStruct((pieces, size, rows, depth), x.dtype), blocks, blocks),
        in_specs=[IN_VMEM] * 3,
        out_specs=[ANY] * 3,
        scratch_shapes=row_gather_scratch(size, pieces) + cube_gather_scratch(ring, 2),
        compiler_params=comm_params(number),
        cost_estimate=comm_cost(COMM_BYTES),
        name="gather_blocks",
    )(x, keys, values)


def scatter_blocks(part, dk, dv, number):
    pieces, size, rows, depth = part.shape
    ring = dk.shape[0]

    def kernel(part_ref, k_ref, v_ref, o_ref, ko_ref, vo_ref, *scratch):
        neighbour_barrier("tp", "ctx")
        run_steps(
            cube_scatter_steps("ctx", (k_ref, v_ref), (ko_ref, vo_ref), *scratch[4:]),
            row_scatter_steps("tp", part_ref, o_ref, *scratch[:4]),
        )

    block = jax.ShapeDtypeStruct(dk.shape[1:], jnp.bfloat16)
    return pl.pallas_call(
        kernel,
        out_shape=(jax.ShapeDtypeStruct((pieces, rows, depth), jnp.float32), block, block),
        in_specs=[IN_VMEM] * 3,
        out_specs=[IN_VMEM] * 3,
        scratch_shapes=row_scatter_scratch(size, (pieces, rows, depth))
        + cube_scatter_scratch(ring, dk.shape[1:], 2),
        compiler_params=comm_params(number),
        cost_estimate=comm_cost(COMM_BYTES),
        name="scatter_blocks",
    )(part, dk, dv)


EPSILON = 1e-05
ROPE_BASE = 130000.0
COMM_BYTES = 64 * 1024 * 1024
MESH = pl.DeviceIdType.MESH


def rope_tables(positions):
    half = HEAD_DIM // 2
    lane = jnp.arange(PAIR, dtype=jnp.int32)
    freq = ROPE_BASE ** (-((lane % half).astype(jnp.float32) * 2.0 / HEAD_DIM))
    angle = positions.astype(jnp.float32)[..., None] * freq
    sign = jnp.where(lane % HEAD_DIM < half, -1.0, 1.0)
    return jnp.cos(angle), jnp.sin(angle) * sign


def body(block_input, block_order, w_qkv, w_out, gain_attn, w_gate_up, w_down, gain_mlp, cotangent):
    f32 = jnp.float32
    bf16 = jnp.bfloat16
    shards = ("dp", "ctx")
    _, pieces, row_count, depth = block_input.shape
    span = row_count * lax.axis_size("tp")
    width = w_qkv.shape[2]
    units = w_gate_up.shape[2]
    shard = w_qkv.shape[0]
    rows = pieces * span
    block_total = block_order.shape[1]
    order = block_order[0]
    first = lax.axis_index("ctx") * pieces
    mine = lax.dynamic_slice_in_dim(order, first, pieces, 0)
    offsets = jnp.arange(span, dtype=jnp.int32)
    cos, sin = rope_tables(order[:, None] * span + offsets)
    qcos, qsin = (
        lax.dynamic_slice_in_dim(t, first, pieces, 0).reshape(rows, PAIR) for t in (cos, sin)
    )

    gain_one = gain_attn.astype(f32)[:, None]
    gain_two = gain_mlp.astype(f32)[:, None]
    flat_qkv = w_qkv.reshape(shard, 3 * width).astype(f32)
    flat_gate_up = w_gate_up.reshape(shard, 2 * units).astype(f32)
    full_qkv = lax.all_gather((flat_qkv * gain_one).astype(bf16), shards, axis=0, tiled=True)
    full_out = lax.all_gather(w_out, shards, axis=1, tiled=True)
    full_gate_up = lax.all_gather(
        (flat_gate_up * gain_two).astype(bf16), shards, axis=0, tiled=True
    )
    full_down = lax.all_gather(w_down, shards, axis=1, tiled=True)

    x = block_input[0].astype(f32)
    rms_attn = lax.rsqrt(jnp.mean(x * x, -1, keepdims=True) + EPSILON)
    unit_attn = x * rms_attn
    unit_attn_full = gather_rows(unit_attn.astype(bf16), 0).reshape(rows, depth)
    queries, keys, values = project(unit_attn_full, full_qkv, qcos, qsin)
    cotan_full, key_blocks, value_blocks = gather_blocks(cotangent[0], keys, values, 1)
    cotan_full = cotan_full.reshape(rows, depth)
    key_blocks = key_blocks.reshape(block_total, span, width)
    value_blocks = value_blocks.reshape(block_total, span, width)
    attention, lse = attend(order, mine, queries, key_blocks, value_blocks)

    def spread(part):
        return part.astype(bf16).reshape(pieces, -1, row_count, depth)

    attn_part = jnp.dot(attention, full_out, preferred_element_type=f32)
    resid_mid = x + scatter_rows(spread(attn_part), 2)
    rms_mlp = lax.rsqrt(jnp.mean(resid_mid * resid_mid, -1, keepdims=True) + EPSILON)
    unit_mlp = resid_mid * rms_mlp
    unit_mlp_full = gather_rows(unit_mlp.astype(bf16), 3).reshape(rows, depth)
    gate_up = jnp.dot(unit_mlp_full, full_gate_up, preferred_element_type=f32)
    gate = gate_up[:, :units]
    upper = gate_up[:, units:]
    sigma = jax.nn.sigmoid(gate)
    hidden = (gate * sigma * upper).astype(bf16)
    grad_hidden = lax.dot_general(cotan_full, full_down, NT, preferred_element_type=f32)
    act_grad = jnp.concatenate(
        [grad_hidden * upper * sigma * (1.0 + gate * (1.0 - sigma)), grad_hidden * gate * sigma],
        axis=1,
    ).astype(bf16)
    grad_down_local = lax.dot_general(hidden, cotan_full, TN, preferred_element_type=f32)
    share_down = lax.psum_scatter(
        grad_down_local.astype(bf16), shards, scatter_dimension=1, tiled=True
    )
    grad_gate_up_local = lax.dot_general(unit_mlp_full, act_grad, TN, preferred_element_type=f32)
    share_gate_up = lax.psum_scatter(
        grad_gate_up_local.astype(bf16), shards, scatter_dimension=0, tiled=True
    )
    scaled_part = lax.dot_general(act_grad, full_gate_up, NT, preferred_element_type=f32)
    scaled_two = scatter_rows(spread(scaled_part), 4)
    cotan = cotangent[0].astype(f32)
    grad_mid = cotan + rms_mlp * (
        scaled_two - unit_mlp * jnp.mean(scaled_two * unit_mlp, -1, keepdims=True)
    )
    mid_full = gather_rows(grad_mid.astype(bf16), 5).reshape(rows, depth)
    grad_attention = lax.dot_general(mid_full, full_out, NT, preferred_element_type=f32)
    grad_queries, key_terms, value_terms = attend_back(
        order, mine, queries, key_blocks, value_blocks, attention, grad_attention.astype(bf16),
        lse, cos, sin, qcos, qsin,
    )
    grad_out_local = lax.dot_general(attention, mid_full, TN, preferred_element_type=f32)
    share_out = lax.psum_scatter(
        grad_out_local.astype(bf16), shards, scatter_dimension=1, tiled=True
    )
    down_part = jnp.dot(hidden, full_down, preferred_element_type=f32)
    down_sum, grad_keys, grad_values = scatter_blocks(
        spread(down_part),
        key_terms.reshape(-1, rows, width),
        value_terms.reshape(-1, rows, width),
        6,
    )
    block_output = (resid_mid + down_sum).astype(bf16)
    qkv_grad = jnp.concatenate([grad_queries, grad_keys, grad_values], axis=1)
    grad_qkv_local = lax.dot_general(unit_attn_full, qkv_grad, TN, preferred_element_type=f32)
    share_qkv = lax.psum_scatter(
        grad_qkv_local.astype(bf16), shards, scatter_dimension=0, tiled=True
    )
    scaled_one_part = lax.dot_general(qkv_grad, full_qkv, NT, preferred_element_type=f32)
    scaled_one = scatter_rows(spread(scaled_one_part), 7)
    input_grad = grad_mid + rms_attn * (
        scaled_one - unit_attn * jnp.mean(scaled_one * unit_attn, -1, keepdims=True)
    )
    raw_qkv = share_qkv.astype(f32)
    raw_gate_up = share_gate_up.astype(f32)
    gain_terms = jnp.stack(
        [jnp.sum(raw_qkv * flat_qkv, -1), jnp.sum(raw_gate_up * flat_gate_up, -1)]
    )
    gain_sums = lax.psum(gain_terms, "tp")
    return (
        block_output[None],
        input_grad[None],
        (raw_qkv * gain_one).reshape(shard, 3, width),
        share_out.astype(f32),
        gain_sums[0],
        (raw_gate_up * gain_two).reshape(shard, 2, units),
        share_down.astype(f32),
        gain_sums[1],
    )


def solution(mesh):
    in_specs = (
        P("dp", "ctx", "tp", None),
        P("dp", None),
        P(("dp", "ctx"), None, "tp"),
        P("tp", ("dp", "ctx")),
        P(("dp", "ctx")),
        P(("dp", "ctx"), None, "tp"),
        P("tp", ("dp", "ctx")),
        P(("dp", "ctx")),
        P("dp", "ctx", "tp", None),
    )
    out_specs = (
        P("dp", "ctx", "tp", None),
        P("dp", "ctx", "tp", None),
        P(("dp", "ctx"), None, "tp"),
        P("tp", ("dp", "ctx")),
        P(("dp", "ctx")),
        P(("dp", "ctx"), None, "tp"),
        P("tp", ("dp", "ctx")),
        P(("dp", "ctx")),
    )
    return jax.shard_map(body, mesh=mesh, in_specs=in_specs, out_specs=out_specs, check_vma=False)
```

```python
import functools

import jax
import jax.numpy as jnp
from jax import lax
from jax.experimental import pallas as pl
from jax.experimental.pallas import tpu as pltpu
from jax.sharding import PartitionSpec as P

HEAD_DIM = 64
PAIR = 2 * HEAD_DIM
NT = (((1,), (1,)), ((), ()))
NN = (((1,), (0,)), ((), ()))
TN = (((0,), (0,)), ((), ()))


def dot(a, b, dims):
    return lax.dot_general(a, b, dims, preferred_element_type=jnp.float32)


def swap_halves(x):
    lane = lax.broadcasted_iota(jnp.int32, x.shape, 1)
    half = HEAD_DIM // 2
    return jnp.where(
        lane % HEAD_DIM < half, pltpu.roll(x, PAIR - half, 1), pltpu.roll(x, half, 1)
    )


def head_part(x, head):
    lane = lax.broadcasted_iota(jnp.int32, x.shape, 1)
    return jnp.where(lane // HEAD_DIM == head, x, jnp.zeros_like(x))


def visible(shape, base, key_off, key_id, query_id, span):
    keys = lax.broadcasted_iota(jnp.int32, shape, 0)
    queries = lax.broadcasted_iota(jnp.int32, shape, 1)
    return keys - queries <= (query_id - key_id) * span


def attend_kernel(order_ref, mine_ref, q_ref, k_ref, v_ref, o_ref, lse_ref, s_ref):
    blocks, span, _ = k_ref.shape
    rows = q_ref.shape[0]
    parts = rows // span

    def one(index, carry):
        head = index // parts
        part = index % parts
        start = pl.multiple_of(part * span, span)
        query = head_part(q_ref[pl.ds(start, span), :], head)
        top = jnp.full((8, span), -1e30, jnp.float32)
        for blk in range(blocks):
            s = dot(k_ref[blk], query, NT)
            seen = visible((span, span), 0, 0, order_ref[blk], mine_ref[part], span)
            s = jnp.where(seen, s, -jnp.inf)
            s_ref[blk] = s
            top = jnp.maximum(top, jnp.max(s.reshape(span // 8, 8, span), 0))
        top = jnp.max(top, 0, keepdims=True)
        total = jnp.zeros((8, span), jnp.float32)
        acc = jnp.zeros((PAIR, span), jnp.float32)
        for blk in range(blocks):
            p = jnp.exp(s_ref[blk] - top)
            total = total + jnp.sum(p.reshape(span // 8, 8, span), 0)
            acc = acc + dot(v_ref[blk], p.astype(jnp.bfloat16), TN)
        total = jnp.sum(total, 0, keepdims=True)
        out = (acc / total).T
        lane = lax.broadcasted_iota(jnp.int32, out.shape, 1)
        old = o_ref[pl.ds(start, span), :]
        o_ref[pl.ds(start, span), :] = jnp.where(
            lane // HEAD_DIM == head, out.astype(o_ref.dtype), old
        )
        lse_ref[0, pl.ds(head * parts + part, 1), :] = top + jnp.log(total)
        return carry

    lax.fori_loop(0, 2 * parts, one, 0)


def attend(order, mine, q, k, v):
    rows, width = q.shape
    blocks, span, _ = k.shape
    pairs = width // PAIR
    parts = rows // span
    return pl.pallas_call(
        attend_kernel,
        out_shape=(
            jax.ShapeDtypeStruct((rows, width), jnp.bfloat16),
            jax.ShapeDtypeStruct((pairs, 2 * parts, span), jnp.float32),
        ),
        grid_spec=pltpu.PrefetchScalarGridSpec(
            num_scalar_prefetch=2,
            grid=(pairs,),
            in_specs=[
                pl.BlockSpec((rows, PAIR), lambda i, *_: (0, i)),
                pl.BlockSpec((blocks, span, PAIR), lambda i, *_: (0, 0, i)),
                pl.BlockSpec((blocks, span, PAIR), lambda i, *_: (0, 0, i)),
            ],
            out_specs=[
                pl.BlockSpec((rows, PAIR), lambda i, *_: (0, i)),
                pl.BlockSpec((1, 2 * parts, span), lambda i, *_: (i, 0, 0)),
            ],
            scratch_shapes=[pltpu.VMEM((blocks, span, span), jnp.float32)],
        ),
        cost_estimate=pl.CostEstimate(
            flops=4 * rows * blocks * span * width * 4,
            bytes_accessed=4 * blocks * span * width + 4 * rows * width,
            transcendentals=rows * blocks * span * width // HEAD_DIM,
        ),
        name="attend",
    )(order, mine, q, k, v)


def attend_back_kernel(
    order_ref, mine_ref, q_ref, k_ref, v_ref, o_ref, g_ref, lse_ref, cos_ref, sin_ref,
    qcos_ref, qsin_ref, dq_ref, dk_ref, dv_ref, dk_acc, dv_acc, dq_acc, kt_ref, delta_ref,
):
    blocks, span, _ = k_ref.shape
    rows = q_ref.shape[0]
    parts = rows // span
    f32 = jnp.float32
    bf16 = jnp.bfloat16
    for blk in range(blocks):
        kt_ref[blk] = k_ref[blk].T
        dk_acc[blk] = jnp.zeros((span, PAIR), f32)
        dv_acc[blk] = jnp.zeros((span, PAIR), f32)
    for part in range(parts):
        take = pl.ds(part * span, span)
        both = (g_ref[take, :].astype(f32) * o_ref[take, :].astype(f32)).T
        for head in range(2):
            delta_ref[pl.ds(head * parts + part, 1), :] = jnp.sum(
                both[head * HEAD_DIM : (head + 1) * HEAD_DIM], 0, keepdims=True
            )
        dq_acc[part] = jnp.zeros((PAIR, span), f32)

    def one(index, carry):
        head = index // parts
        part = index % parts
        start = pl.multiple_of(part * span, span)
        query = head_part(q_ref[pl.ds(start, span), :], head)
        grad = head_part(g_ref[pl.ds(start, span), :], head)
        lse = lse_ref[0, pl.ds(index, 1), :]
        delta = delta_ref[pl.ds(index, 1), :]
        dq = jnp.zeros((PAIR, span), f32)
        for blk in range(blocks):
            s = dot(k_ref[blk], query, NT)
            seen = visible((span, span), 0, 0, order_ref[blk], mine_ref[part], span)
            p = jnp.exp(jnp.where(seen, s - lse, -jnp.inf))
            dp = dot(v_ref[blk], grad, NT)
            ds = (p * (dp - delta)).astype(bf16)
            dv_acc[blk] += dot(p.astype(bf16), grad, NN)
            dk_acc[blk] += dot(ds, query, NN)
            dq = dq + dot(kt_ref[blk], ds, NN)
        sub = lax.broadcasted_iota(jnp.int32, dq.shape, 0)
        dq_acc[part] += jnp.where(sub // HEAD_DIM == head, dq, 0.0)
        return carry

    lax.fori_loop(0, 2 * parts, one, 0)
    for part in range(parts):
        take = pl.ds(part * span, span)
        dq = dq_acc[part].T
        dq = dq * qcos_ref[take, :] - swap_halves(dq) * qsin_ref[take, :]
        dq_ref[take, :] = (dq * 0.125).astype(bf16)
    for blk in range(blocks):
        dk = dk_acc[blk]
        dk = dk * cos_ref[blk] - swap_halves(dk) * sin_ref[blk]
        dk_ref[blk] = dk.astype(bf16)
        dv_ref[blk] = dv_acc[blk].astype(bf16)


def attend_back(order, mine, q, k, v, o, g, lse, cos, sin, qcos, qsin):
    rows, width = q.shape
    blocks, span, _ = k.shape
    pairs = width // PAIR
    parts = rows // span
    row_spec = pl.BlockSpec((rows, PAIR), lambda i, *_: (0, i))
    blk_spec = pl.BlockSpec((blocks, span, PAIR), lambda i, *_: (0, 0, i))
    tab_spec = pl.BlockSpec((blocks, span, PAIR), lambda i, *_: (0, 0, 0))
    qtab_spec = pl.BlockSpec((rows, PAIR), lambda i, *_: (0, 0))
    f32 = jnp.float32
    return pl.pallas_call(
        attend_back_kernel,
        out_shape=(
            jax.ShapeDtypeStruct((rows, width), jnp.bfloat16),
            jax.ShapeDtypeStruct((blocks, span, width), jnp.bfloat16),
            jax.ShapeDtypeStruct((blocks, span, width), jnp.bfloat16),
        ),
        grid_spec=pltpu.PrefetchScalarGridSpec(
            num_scalar_prefetch=2,
            grid=(pairs,),
            in_specs=[
                row_spec, blk_spec, blk_spec, row_spec, row_spec,
                pl.BlockSpec((1, 2 * parts, span), lambda i, *_: (i, 0, 0)),
                tab_spec, tab_spec, qtab_spec, qtab_spec,
            ],
            out_specs=[row_spec, blk_spec, blk_spec],
            scratch_shapes=[
                pltpu.VMEM((blocks, span, PAIR), f32),
                pltpu.VMEM((blocks, span, PAIR), f32),
                pltpu.VMEM((parts, PAIR, span), f32),
                pltpu.VMEM((blocks, PAIR, span), jnp.bfloat16),
                pltpu.VMEM((2 * parts, span), f32),
            ],
        ),
        cost_estimate=pl.CostEstimate(
            flops=10 * rows * blocks * span * width * 4,
            bytes_accessed=8 * blocks * span * width + 8 * rows * width,
            transcendentals=rows * blocks * span * width // HEAD_DIM,
        ),
        name="attend_back",
    )(order, mine, q, k, v, o, g, lse, cos, sin, qcos, qsin)


def project_kernel(x_ref, w_ref, cos_ref, sin_ref, q_ref, k_ref, v_ref):
    which = pl.program_id(0)
    out = dot(x_ref[...], w_ref[...], NN)

    def turned(scale, ref):
        for lane in range(0, out.shape[1], PAIR):
            piece = out[:, lane : lane + PAIR]
            piece = piece * cos_ref[...] + swap_halves(piece) * sin_ref[...]
            ref[:, lane : lane + PAIR] = (piece * scale).astype(ref.dtype)

    @pl.when(which == 0)
    def _():
        turned(0.125, q_ref)

    @pl.when(which == 1)
    def _():
        turned(1.0, k_ref)

    @pl.when(which == 2)
    def _():
        v_ref[...] = out.astype(v_ref.dtype)


def project(x, w, qcos, qsin):
    rows, depth = x.shape
    width = w.shape[1] // 3
    whole = lambda shape: pl.BlockSpec(shape, lambda t: (0,) * len(shape))
    out = jax.ShapeDtypeStruct((rows, width), jnp.bfloat16)
    return pl.pallas_call(
        project_kernel,
        out_shape=(out, out, out),
        grid=(3,),
        in_specs=[
            whole((rows, depth)),
            pl.BlockSpec((depth, width), lambda t: (0, t)),
            whole((rows, PAIR)),
            whole((rows, PAIR)),
        ],
        out_specs=[whole((rows, width))] * 3,
        cost_estimate=pl.CostEstimate(
            flops=2 * rows * depth * 3 * width,
            bytes_accessed=2 * depth * 3 * width + 2 * rows * depth,
            transcendentals=0,
        ),
        name="project",
    )(x, w, qcos, qsin)


def cube_size(axes):
    size = 1
    for axis in axes:
        size *= lax.axis_size(axis)
    return size


def cube_index(axes):
    index = 0
    for axis in axes:
        index = index * lax.axis_size(axis) + lax.axis_index(axis)
    return index


def cube_bits(size):
    bits = []
    while size > 1:
        size //= 2
        bits.append(size)
    return bits


def flipped(index, bit):
    return index + bit - 2 * bit * ((index // bit) % 2)


def flip_all(index, mask):
    bit = 1
    while bit <= mask:
        if mask // bit % 2:
            index = flipped(index, bit)
        bit *= 2
    return index


def cube_peer(axes, bit):
    for axis in axes[::-1]:
        size = lax.axis_size(axis)
        if bit < size:
            return {axis: flipped(lax.axis_index(axis), bit)}
        bit //= size
    raise ValueError(bit)


def greet(line_axis, cube_axes):
    sem = pltpu.get_barrier_semaphore()
    count = 0

    def hello(target):
        pl.semaphore_signal(sem, inc=1, device_id=target, device_id_type=MESH)

    if line_axis is not None:
        me = lax.axis_index(line_axis)
        size = lax.axis_size(line_axis)

        @pl.when(me > 0)
        def _():
            hello({line_axis: me - 1})

        @pl.when(me < size - 1)
        def _():
            hello({line_axis: me + 1})

    if cube_axes is not None:
        for bit in cube_bits(cube_size(cube_axes)):
            hello(cube_peer(cube_axes, bit))
            count += 1
    if line_axis is not None:

        @pl.when((me > 0) & (me < size - 1))
        def _():
            pl.semaphore_wait(sem, count + 2)

        @pl.when((me == 0) | (me == size - 1))
        def _():
            pl.semaphore_wait(sem, count + 1)

    else:
        pl.semaphore_wait(sem, count)


def remote(src, dst, send, recv, target):
    return pltpu.make_async_remote_copy(
        src_ref=src, dst_ref=dst, send_sem=send, recv_sem=recv,
        device_id=target, device_id_type=MESH,
    )


class RowGather:
    def __init__(self, axis, x_ref, o_ref, send, recv, local):
        self.axis, self.x, self.o = axis, x_ref, o_ref
        self.send, self.recv, self.local = send, recv, local
        self.size = lax.axis_size(axis)
        self.me = lax.axis_index(axis)
        self.pieces = x_ref.shape[0]

    @staticmethod
    def scratch(size, pieces):
        return [
            pltpu.SemaphoreType.DMA((2, size - 1, pieces)),
            pltpu.SemaphoreType.DMA((2, size - 1, pieces)),
            pltpu.SemaphoreType.DMA((pieces,)),
        ]

    def peer(self, way):
        return {self.axis: self.me + 1 if way == 0 else self.me - 1}

    def own(self, p):
        return pltpu.make_async_copy(self.x.at[p], self.o.at[p, self.me], self.local.at[p])

    def copy(self, way, step, p):
        block = self.me - step if way == 0 else self.me + step
        src = self.x.at[p] if step == 0 else self.o.at[p, block]
        return remote(
            src, self.o.at[p, block], self.send.at[way, step, p], self.recv.at[way, step, p],
            self.peer(way),
        )

    def sends(self, way, step):
        if way == 0:
            return (self.me < self.size - 1) & (self.me - step >= 0)
        return (self.me > 0) & (self.me + step < self.size)

    def arrives(self, way, step):
        return self.me - 1 - step >= 0 if way == 0 else self.me + 1 + step < self.size

    def arrival(self, way, step, p):
        block = self.me - 1 - step if way == 0 else self.me + 1 + step
        return remote(
            self.o.at[p, block], self.o.at[p, block], self.send.at[way, step, p],
            self.recv.at[way, step, p], self.peer(1 - way),
        )

    def start(self, p):
        for way in (0, 1):

            @pl.when(self.sends(way, 0))
            def _(way=way):
                self.copy(way, 0, p).start()

        self.own(p).start()

    def flow(self):
        for step in range(1, self.size):
            for p in range(self.pieces):
                for way in (0, 1):

                    @pl.when(self.arrives(way, step - 1))
                    def _(way=way, p=p):
                        self.arrival(way, step - 1, p).wait_recv()

                    if step < self.size - 1:

                        @pl.when(self.sends(way, step))
                        def _(way=way, p=p):
                            self.copy(way, step, p).start()

            yield
        for p in range(self.pieces):
            self.own(p).wait()
        for step in range(self.size - 1):
            for way in (0, 1):

                @pl.when(self.sends(way, step))
                def _(way=way, step=step):
                    for p in range(self.pieces):
                        self.copy(way, step, p).wait_send()

    def steps(self):
        for p in range(self.pieces):
            self.start(p)
        yield
        yield from self.flow()


class RowScatter:
    def __init__(self, axis, part_ref, inbox, outbox, send, recv):
        self.axis, self.part, self.inbox, self.outbox = axis, part_ref, inbox, outbox
        self.send, self.recv = send, recv
        self.size = lax.axis_size(axis)
        self.me = lax.axis_index(axis)
        self.pieces = part_ref.shape[0]

    @staticmethod
    def scratch(size, block):
        return [
            pltpu.VMEM((2, size - 1) + block, jnp.bfloat16),
            pltpu.VMEM((2, size - 1) + block, jnp.bfloat16),
            pltpu.SemaphoreType.DMA((2, size - 1, block[0])),
            pltpu.SemaphoreType.DMA((2, size - 1, block[0])),
        ]

    def peer(self, way):
        return {self.axis: self.me + 1 if way == 0 else self.me - 1}

    def target(self, way, step):
        return self.size - 1 - step if way == 0 else step

    def edge(self, way):
        return self.me == 0 if way == 0 else self.me == self.size - 1

    def inner(self, way):
        return self.me > 0 if way == 0 else self.me < self.size - 1

    def passes(self, way, step):
        dest = self.target(way, step)
        return dest > self.me if way == 0 else dest < self.me

    def copy(self, way, step, p, edge):
        src = self.part.at[p, self.target(way, step)] if edge else self.outbox.at[way, step, p]
        return remote(
            src, self.inbox.at[way, step, p], self.send.at[way, step, p],
            self.recv.at[way, step, p], self.peer(way),
        )

    def arrival(self, way, step, p):
        return remote(
            self.inbox.at[way, step, p], self.inbox.at[way, step, p],
            self.send.at[way, step, p], self.recv.at[way, step, p], self.peer(1 - way),
        )

    def flow(self):
        f32 = jnp.float32
        for way in (0, 1):

            @pl.when(self.edge(way))
            def _(way=way):
                for step in range(self.size - 1):
                    for p in range(self.pieces):
                        self.copy(way, step, p, True).start()

        yield
        for step in range(self.size - 1):
            for p in range(self.pieces):
                for way in (0, 1):

                    @pl.when(self.passes(way, step) & self.inner(way))
                    def _(way=way, step=step, p=p):
                        self.arrival(way, step, p).wait_recv()
                        self.outbox[way, step, p] = (
                            self.inbox[way, step, p].astype(f32)
                            + self.part[p, self.target(way, step)].astype(f32)
                        ).astype(self.outbox.dtype)
                        self.copy(way, step, p, False).start()

            yield

    def collect(self, p, o_ref):
        f32 = jnp.float32
        o_ref[p] = self.part[p, self.me].astype(f32)
        for way in (0, 1):

            @pl.when(self.inner(way))
            def _(way=way):
                step = self.size - 1 - self.me if way == 0 else self.me
                self.arrival(way, step, p).wait_recv()
                o_ref[p] += self.inbox[way, step, p].astype(f32)

    def finish(self):
        for step in range(self.size - 1):
            for way in (0, 1):

                @pl.when(self.passes(way, step))
                def _(way=way, step=step):
                    for p in range(self.pieces):
                        self.copy(way, step, p, False).wait_send()

    def steps(self, o_ref):
        yield from self.flow()
        for p in range(self.pieces):
            self.collect(p, o_ref)
        yield
        self.finish()


def cube_gather_steps(axes, count, source, place, send, recv, local):
    size = cube_size(axes)
    me = cube_index(axes)
    bits = cube_bits(size)
    own = [
        pltpu.make_async_copy(source(t), place(t, me), local.at[t]) for t in range(count)
    ]

    def copy(mask, bit, t):
        block = flip_all(me, mask)
        src = source(t) if mask == 0 else place(t, block)
        return remote(
            src, place(t, block), send.at[mask + bit, t], recv.at[mask + bit, t],
            cube_peer(axes, bit),
        )

    def arrival(mask, t):
        place_here = place(t, flip_all(me, mask))
        return remote(
            place_here, place_here, send.at[mask, t], recv.at[mask, t],
            cube_peer(axes, mask & -mask),
        )

    for bit in bits:
        for t in range(count):
            copy(0, bit, t).start()
    for one in own:
        one.start()
    yield
    waited = set()
    masks = [0]
    for bit in bits:
        for mask in masks:
            if mask == 0:
                continue
            for t in range(count):
                if (mask, t) not in waited:
                    arrival(mask, t).wait_recv()
                    waited.add((mask, t))
                copy(mask, bit, t).start()
            yield
        masks = masks + [mask + bit for mask in masks]
    for mask in masks:
        for t in range(count):
            if mask and (mask, t) not in waited:
                arrival(mask, t).wait_recv()
    for one in own:
        one.wait()
    for mask in masks:
        for t in range(count):
            if mask:
                low = mask & -mask
                copy(mask - low, low, t).wait_send()


def cube_gather_scratch(size, count):
    return [
        pltpu.SemaphoreType.DMA((size, count)),
        pltpu.SemaphoreType.DMA((size, count)),
        pltpu.SemaphoreType.DMA((count,)),
    ]


def cube_scatter_steps(axes, parts, inbox, total, outbox, send, recv, done):
    size = cube_size(axes)
    me = cube_index(axes)
    bits = cube_bits(size)[::-1]
    count = len(parts)
    f32 = jnp.float32
    order = sorted(range(size), key=lambda mask: tuple(-(mask & bit) for bit in bits))

    def copy(mask, t):
        bit = mask & -mask
        src = parts[t].at[flip_all(me, mask)] if bit == 1 else outbox.at[mask // 2, t]
        return remote(
            src, inbox.at[mask, t], send.at[mask, t], recv.at[mask, t], cube_peer(axes, bit)
        )

    for mask in order:
        if mask & 1:
            for t in range(count):
                copy(mask, t).start()
    yield
    for level, bit in enumerate(bits):
        after = bits[level + 1] if level + 1 < len(bits) else 0
        for mask in order:
            if mask % (2 * bit):
                continue
            for t in range(count):
                copy(mask + bit, t).wait_recv()
                if bit == 1:
                    base = parts[t][flip_all(me, mask)].astype(f32)
                else:
                    base = total[mask // 4, t]
                value = base + inbox[mask + bit, t].astype(f32)
                if mask & after:
                    outbox[mask // 2, t] = value.astype(outbox.dtype)
                    copy(mask, t).start()
                elif after:
                    total[mask // 4, t] = value
                else:
                    done(t, value)
            yield
    for mask in range(1, size):
        for t in range(count):
            copy(mask, t).wait_send()


def cube_scatter_scratch(size, block, count):
    return [
        pltpu.VMEM((size, count) + block, jnp.bfloat16),
        pltpu.VMEM((max(size // 4, 1), count) + block, jnp.float32),
        pltpu.VMEM((max(size // 2, 1), count) + block, jnp.bfloat16),
        pltpu.SemaphoreType.DMA((size, count)),
        pltpu.SemaphoreType.DMA((size, count)),
    ]


def run_steps(walks, order=()):
    walks = list(walks)
    for index in order:
        next(walks[index], None)
    while walks:
        for walk in list(walks):
            try:
                next(walk)
            except StopIteration:
                walks.remove(walk)


ANY = pl.BlockSpec(memory_space=pl.ANY)
IN_VMEM = pl.BlockSpec(memory_space=pltpu.VMEM)


def comm_call(kernel, number, size, **kwargs):
    return pl.pallas_call(
        kernel,
        compiler_params=pltpu.CompilerParams(
            collective_id=number, has_side_effects=True, vmem_limit_bytes=52 * 1024 * 1024
        ),
        cost_estimate=pl.CostEstimate(flops=0, bytes_accessed=size, transcendentals=0),
        **kwargs,
    )


def enter(x, w, number):
    pieces, rows, depth = x.shape
    size = lax.axis_size("tp")
    shards = ("dp", "ctx")
    group = cube_size(shards)
    cuts = 2
    part = w.shape[0] // cuts

    def kernel(x_ref, w_ref, o_ref, wo_ref, *sems):
        greet("tp", shards)
        take = lambda t: pl.ds(t * part, part)
        run_steps(
            (
                RowGather("tp", x_ref, o_ref, *sems[:3]).steps(),
                cube_gather_steps(
                    shards, cuts, lambda t: w_ref.at[take(t)],
                    lambda t, block: wo_ref.at[block, take(t)], *sems[3:],
                ),
            )
        )

    return comm_call(
        kernel, number, COMM_BYTES,
        out_shape=(
            jax.ShapeDtypeStruct((pieces, size, rows, depth), x.dtype),
            jax.ShapeDtypeStruct((group,) + w.shape, w.dtype),
        ),
        in_specs=[IN_VMEM] * 2,
        out_specs=[ANY] * 2,
        scratch_shapes=RowGather.scratch(size, pieces) + cube_gather_scratch(group, cuts),
        name="enter",
    )(x, w)


def gather_blocks(x, keys, values, number):
    pieces, rows, depth = x.shape
    size = lax.axis_size("tp")
    ring = lax.axis_size("ctx")

    def kernel(x_ref, k_ref, v_ref, o_ref, ko_ref, vo_ref, *sems):
        greet("tp", ("ctx",))
        ins, outs = (k_ref, v_ref), (ko_ref, vo_ref)
        run_steps(
            (
                cube_gather_steps(
                    ("ctx",), 2, lambda t: ins[t], lambda t, block: outs[t].at[block], *sems[3:]
                ),
                RowGather("tp", x_ref, o_ref, *sems[:3]).steps(),
            )
        )

    blocks = jax.ShapeDtypeStruct((ring,) + keys.shape, keys.dtype)
    return comm_call(
        kernel, number, COMM_BYTES,
        out_shape=(jax.ShapeDtypeStruct((pieces, size, rows, depth), x.dtype), blocks, blocks),
        in_specs=[IN_VMEM] * 3,
        out_specs=[ANY] * 3,
        scratch_shapes=RowGather.scratch(size, pieces) + cube_gather_scratch(ring, 2),
        name="gather_blocks",
    )(x, keys, values)


def mix_rows(part, sides, finish, number, name):
    pieces, size, rows, depth = part.shape
    count = len(sides)

    def kernel(part_ref, *refs):
        side_refs, (sum_ref, o_ref), refs = refs[:count], refs[count : count + 2], refs[count + 2 :]
        own_ref, scatter_scratch, sems = refs[0], refs[1:5], refs[5:]
        greet("tp", None)
        scatter = RowScatter("tp", part_ref, *scatter_scratch)
        gather = RowGather("tp", own_ref, o_ref, *sems)
        run_steps((scatter.flow(),))
        for p in range(pieces):
            scatter.collect(p, sum_ref)
            kept, sent = finish(sum_ref[p], *(ref[p] for ref in side_refs))
            sum_ref[p] = kept
            own_ref[p] = sent.astype(own_ref.dtype)
            gather.start(p)
        run_steps((gather.flow(),))
        scatter.finish()

    return comm_call(
        kernel, number, 2 * COMM_BYTES,
        out_shape=(
            jax.ShapeDtypeStruct((pieces, rows, depth), jnp.float32),
            jax.ShapeDtypeStruct((pieces, size, rows, depth), jnp.bfloat16),
        ),
        in_specs=[IN_VMEM] * (1 + count),
        out_specs=[IN_VMEM, ANY],
        scratch_shapes=[pltpu.VMEM((pieces, rows, depth), jnp.bfloat16)]
        + RowScatter.scratch(size, (pieces, rows, depth))
        + RowGather.scratch(size, pieces),
        name=name,
    )(part, *sides)


def scatter_blocks(part, dk, dv, number):
    pieces, size, rows, depth = part.shape
    ring = dk.shape[0]

    def kernel(part_ref, k_ref, v_ref, o_ref, ko_ref, vo_ref, *scratch):
        greet("tp", ("ctx",))
        outs = (ko_ref, vo_ref)

        def done(t, value):
            outs[t][...] = value.astype(outs[t].dtype)

        run_steps(
            (
                RowScatter("tp", part_ref, *scratch[:4]).steps(o_ref),
                cube_scatter_steps(("ctx",), (k_ref, v_ref), *scratch[4:], done),
            ),
            (0, 1, 1, 1, 0, 0),
        )

    block = jax.ShapeDtypeStruct(dk.shape[1:], jnp.bfloat16)
    return comm_call(
        kernel, number, COMM_BYTES,
        out_shape=(jax.ShapeDtypeStruct((pieces, rows, depth), jnp.float32), block, block),
        in_specs=[IN_VMEM] * 3,
        out_specs=[IN_VMEM] * 3,
        scratch_shapes=RowScatter.scratch(size, (pieces, rows, depth))
        + cube_scatter_scratch(ring, dk.shape[1:], 2),
        name="scatter_blocks",
    )(part, dk, dv)


def leave(part, grad, number):
    pieces, size, rows, depth = part.shape
    shards = ("dp", "ctx")
    group = cube_size(shards)
    block = grad.shape[1:]

    def kernel(part_ref, g_ref, o_ref, go_ref, *scratch):
        greet("tp", shards)

        def done(t, value):
            go_ref[...] = value

        run_steps(
            (
                RowScatter("tp", part_ref, *scratch[:4]).steps(o_ref),
                cube_scatter_steps(shards, (g_ref,), *scratch[4:], done),
            ),
            (0,) + (1,) * (1 + group // 2) + (0, 0, 1),
        )

    return comm_call(
        kernel, number, COMM_BYTES,
        out_shape=(
            jax.ShapeDtypeStruct((pieces, rows, depth), jnp.float32),
            jax.ShapeDtypeStruct(block, jnp.float32),
        ),
        in_specs=[IN_VMEM] * 2,
        out_specs=[IN_VMEM] * 2,
        scratch_shapes=RowScatter.scratch(size, (pieces, rows, depth))
        + cube_scatter_scratch(group, block, 1),
        name="leave",
    )(part, grad)


def sum_small(x, number):
    size = lax.axis_size("tp")

    def kernel(x_ref, o_ref, inbox, send, recv):
        me = lax.axis_index("tp")
        sem = pltpu.get_barrier_semaphore()
        for step in range(1, size):
            pl.semaphore_signal(
                sem, inc=1, device_id={"tp": (me + step) % size}, device_id_type=MESH
            )
        pl.semaphore_wait(sem, size - 1)
        copies = [
            remote(
                x_ref, inbox.at[step - 1], send.at[step - 1], recv.at[step - 1],
                {"tp": (me + step) % size},
            )
            for step in range(1, size)
        ]
        for copy in copies:
            copy.start()
        total = x_ref[...]
        for step, copy in enumerate(copies):
            copy.wait()
            total = total + inbox[step]
        o_ref[...] = total

    return comm_call(
        kernel, number, x.size * 4,
        out_shape=jax.ShapeDtypeStruct(x.shape, x.dtype),
        in_specs=[IN_VMEM],
        out_specs=IN_VMEM,
        scratch_shapes=[
            pltpu.VMEM((size - 1,) + x.shape, x.dtype),
            pltpu.SemaphoreType.DMA((size - 1,)),
            pltpu.SemaphoreType.DMA((size - 1,)),
        ],
        name="sum_small",
    )(x)


EPSILON = 1e-05
ROPE_BASE = 130000.0
COMM_BYTES = 128 * 1024 * 1024
MESH = pl.DeviceIdType.MESH


def rope_tables(positions):
    half = HEAD_DIM // 2
    lane = jnp.arange(PAIR, dtype=jnp.int32)
    freq = ROPE_BASE ** (-((lane % half).astype(jnp.float32) * 2.0 / HEAD_DIM))
    angle = positions.astype(jnp.float32)[..., None] * freq
    sign = jnp.where(lane % HEAD_DIM < half, -1.0, 1.0)
    return jnp.cos(angle), jnp.sin(angle) * sign


def body(block_input, block_order, w_qkv, w_out, gain_attn, w_gate_up, w_down, gain_mlp, cotangent):
    f32 = jnp.float32
    bf16 = jnp.bfloat16
    shards = ("dp", "ctx")
    _, pieces, row_count, depth = block_input.shape
    span = row_count * lax.axis_size("tp")
    width = w_qkv.shape[2]
    units = w_gate_up.shape[2]
    shard = w_qkv.shape[0]
    rows = pieces * span
    block_total = block_order.shape[1]
    order = block_order[0]
    first = lax.axis_index("ctx") * pieces
    mine = lax.dynamic_slice_in_dim(order, first, pieces, 0)
    offsets = jnp.arange(span, dtype=jnp.int32)
    cos, sin = rope_tables(order[:, None] * span + offsets)
    qcos, qsin = (
        lax.dynamic_slice_in_dim(t, first, pieces, 0).reshape(rows, PAIR) for t in (cos, sin)
    )

    gain_one = gain_attn.astype(f32)[:, None]
    gain_two = gain_mlp.astype(f32)[:, None]
    flat_qkv = w_qkv.reshape(shard, 3 * width).astype(f32)
    flat_gate_up = w_gate_up.reshape(shard, 2 * units).astype(f32)
    x = block_input[0].astype(f32)
    rms_attn = lax.rsqrt(jnp.mean(x * x, -1, keepdims=True) + EPSILON)
    unit_attn = x * rms_attn
    unit_attn_full, full_qkv = enter(
        unit_attn.astype(bf16), (flat_qkv * gain_one).astype(bf16), 0
    )
    unit_attn_full = unit_attn_full.reshape(rows, depth)
    full_qkv = full_qkv.reshape(depth, 3 * width)
    own_out, own_gate_up, own_down, unit_attn_full = lax.optimization_barrier(
        (w_out, (flat_gate_up * gain_two).astype(bf16), w_down, unit_attn_full)
    )
    full_out = lax.all_gather(own_out, shards, axis=1, tiled=True)
    full_gate_up = lax.all_gather(own_gate_up, shards, axis=0, tiled=True)
    full_down = lax.all_gather(own_down, shards, axis=1, tiled=True)
    queries, keys, values = project(unit_attn_full, full_qkv, qcos, qsin)
    cotan_full, key_blocks, value_blocks = gather_blocks(cotangent[0], keys, values, 1)
    cotan_full = cotan_full.reshape(rows, depth)
    key_blocks = key_blocks.reshape(block_total, span, width)
    value_blocks = value_blocks.reshape(block_total, span, width)
    attention, lse = attend(order, mine, queries, key_blocks, value_blocks)

    def spread(part):
        return part.astype(bf16).reshape(pieces, -1, row_count, depth)

    attn_part = jnp.dot(attention, full_out, preferred_element_type=f32)

    def norm_mlp(total, own):
        resid = own.astype(f32) + total
        return resid, resid * lax.rsqrt(jnp.mean(resid * resid, -1, keepdims=True) + EPSILON)

    resid_mid, unit_mlp_full = mix_rows(
        spread(attn_part), (block_input[0],), norm_mlp, 2, "mix_forward"
    )
    unit_mlp_full = unit_mlp_full.reshape(rows, depth)
    gate_up = jnp.dot(unit_mlp_full, full_gate_up, preferred_element_type=f32)
    gate = gate_up[:, :units]
    upper = gate_up[:, units:]
    sigma = jax.nn.sigmoid(gate)
    hidden = (gate * sigma * upper).astype(bf16)
    grad_hidden = lax.dot_general(cotan_full, full_down, NT, preferred_element_type=f32)
    act_grad = jnp.concatenate(
        [grad_hidden * upper * sigma * (1.0 + gate * (1.0 - sigma)), grad_hidden * gate * sigma],
        axis=1,
    ).astype(bf16)
    grad_down_local = lax.dot_general(
        hidden, cotan_full, TN, preferred_element_type=f32
    ).astype(bf16)
    share_down = lax.psum_scatter(grad_down_local, shards, scatter_dimension=1, tiled=True)
    grad_gate_up_local = lax.dot_general(
        unit_mlp_full, act_grad, TN, preferred_element_type=f32
    ).astype(bf16)
    share_gate_up = lax.psum_scatter(grad_gate_up_local, shards, scatter_dimension=0, tiled=True)
    scaled_part = lax.dot_general(act_grad, full_gate_up, NT, preferred_element_type=f32)
    scaled_part, _, _ = lax.optimization_barrier(
        (spread(scaled_part), grad_down_local, grad_gate_up_local)
    )

    def norm_back(total, resid, own):
        rms = lax.rsqrt(jnp.mean(resid * resid, -1, keepdims=True) + EPSILON)
        unit = resid * rms
        grad = own.astype(f32) + rms * (total - unit * jnp.mean(total * unit, -1, keepdims=True))
        return grad, grad

    grad_mid, mid_full = mix_rows(
        scaled_part, (resid_mid, cotangent[0]), norm_back, 3, "mix_backward"
    )
    mid_full = mid_full.reshape(rows, depth)
    grad_attention = lax.dot_general(mid_full, full_out, NT, preferred_element_type=f32)
    grad_queries, key_terms, value_terms = attend_back(
        order, mine, queries, key_blocks, value_blocks, attention, grad_attention.astype(bf16),
        lse, cos, sin, qcos, qsin,
    )
    grad_out_local = lax.dot_general(attention, mid_full, TN, preferred_element_type=f32)
    share_out = lax.psum_scatter(
        grad_out_local.astype(bf16), shards, scatter_dimension=1, tiled=True
    )
    down_part = jnp.dot(hidden, full_down, preferred_element_type=f32)
    down_sum, grad_keys, grad_values = scatter_blocks(
        spread(down_part),
        key_terms.reshape(-1, rows, width),
        value_terms.reshape(-1, rows, width),
        4,
    )
    block_output = (resid_mid + down_sum).astype(bf16)
    qkv_grad = jnp.concatenate([grad_queries, grad_keys, grad_values], axis=1)
    grad_qkv_local = lax.dot_general(unit_attn_full, qkv_grad, TN, preferred_element_type=f32)
    scaled_one_part = lax.dot_general(qkv_grad, full_qkv, NT, preferred_element_type=f32)
    scaled_one, raw_qkv = leave(
        spread(scaled_one_part), grad_qkv_local.astype(bf16).reshape(-1, shard, 3 * width), 5
    )
    input_grad = grad_mid + rms_attn * (
        scaled_one - unit_attn * jnp.mean(scaled_one * unit_attn, -1, keepdims=True)
    )
    raw_gate_up = share_gate_up.astype(f32)
    gain_terms = jnp.stack(
        [jnp.sum(raw_qkv * flat_qkv, -1), jnp.sum(raw_gate_up * flat_gate_up, -1)]
    )
    gain_sums = sum_small(gain_terms, 6)
    return (
        block_output[None],
        input_grad[None],
        (raw_qkv * gain_one).reshape(shard, 3, width),
        share_out.astype(f32),
        gain_sums[0],
        (raw_gate_up * gain_two).reshape(shard, 2, units),
        share_down.astype(f32),
        gain_sums[1],
    )


def solution(mesh):
    in_specs = (
        P("dp", "ctx", "tp", None),
        P("dp", None),
        P(("dp", "ctx"), None, "tp"),
        P("tp", ("dp", "ctx")),
        P(("dp", "ctx")),
        P(("dp", "ctx"), None, "tp"),
        P("tp", ("dp", "ctx")),
        P(("dp", "ctx")),
        P("dp", "ctx", "tp", None),
    )
    out_specs = (
        P("dp", "ctx", "tp", None),
        P("dp", "ctx", "tp", None),
        P(("dp", "ctx"), None, "tp"),
        P("tp", ("dp", "ctx")),
        P(("dp", "ctx")),
        P(("dp", "ctx"), None, "tp"),
        P("tp", ("dp", "ctx")),
        P(("dp", "ctx")),
    )
    return jax.shard_map(body, mesh=mesh, in_specs=in_specs, out_specs=out_specs, check_vma=False)
```
